256 devices in a mesh: occ: 8 (over x, z_hi), vir: 8 (over z_lo, core), aux: 4 (over y).
Axes of the slice: x: 4, y: 4, z: 8 (z_hi: 2, z_lo: 4; z = z_hi * 4 + z_lo), core: 2. Of those that a mesh axis runs over, the one named last changes fastest.
Arguments:
- amplitudes: bfloat16 [64, 1024, 1024], P('occ', 'vir'), may hold values from -6 to 6
- pair_mask: int32 [64, 8, 8], P('occ', 'vir'), may hold values 0 or 1
- left_factor: bfloat16 [32, 1024, 4096], P(None, 'vir', 'aux'), may hold values from -0.0390625 to 0.0390625
- left_mask: int32 [8, 32], P('vir', 'aux'), may hold values 0 or 1
- right_factor: bfloat16 [1024, 4, 4096], P(('occ', 'vir'), None, 'aux'), may hold values from -0.0390625 to 0.0390625
- right_mask: int32 [8, 32], P(None, 'aux'), may hold values 0 or 1
- residual_in: float32 [64, 4, 32], P('occ'), may hold values from -6 to 6
Outputs:
- updated: float32 [64, 4, 32], P('occ')
The draws below stay inside these ranges and needn't reach their ends.
All inputs are finite; a program needn't handle non-finite values. No bound on the sum of `pair_mask` or of `left_mask` or of `right_mask` on one device may be relied on, other than what follows from the above.
Results may differ from the reference program's by a relative error of at most 0.0003.
Values may be sent and summed in bfloat16 or wider, within the bound.
A program may use at most 128 MiB of HBM per device.

```python
import jax
import jax.numpy as jnp
from jax import lax

V = 1024
NAUX = 4096
TILE = 128
AW = 32
BW = 4
PAIRS = 64
NVT = 8
NQT = 32


def set_ends(entries, own_key, smallest, top_value):
    dims = entries.shape
    place = [jax.random.randint(jax.random.fold_in(own_key, axis), (), 0, dims[axis]) for axis in range(len(dims))]
    entries = entries.at[tuple(place)].set(smallest)
    longest = dims.index(max(dims))
    place[longest] = (place[longest] + 1) % dims[longest]
    return entries.at[tuple(place)].set(top_value)


def block_levels(rng, dims, cuts, low, high):
    def one(dim, parts):
        draws = jax.random.uniform(jax.random.fold_in(jax.random.fold_in(rng, 6), dim), (parts,), jnp.float32, low / len(cuts), high / len(cuts))
        return jnp.repeat(jnp.exp(draws), dims[dim] // parts).reshape((-1,) + (1,) * (len(dims) - dim - 1))

    level = one(*cuts[0])
    for cut in cuts[1:]:
        level = level * one(*cut)
    return level


def scatter_about(rng, shape, spread, bound, split=(), kind=jnp.bfloat16):
    drawn = spread * jax.random.normal(rng, shape, jnp.float32)
    if split:
        drawn = drawn * block_levels(rng, shape, split, -0.22, 0.18)
    return jnp.clip(drawn, -bound, bound).astype(kind)


def setup_inputs(seed: int = 0) -> dict:
    key_list = jax.random.split(jax.random.key(seed), 8)
    return {
        "amplitudes": scatter_about(key_list[0], (PAIRS, V, V), 1.0, 6.0, ((0, 8), (1, 8))),
        "pair_mask": set_ends((jax.random.randint(key_list[1], (PAIRS, NVT, NVT), 0, 4) < 3).astype(jnp.int32), jax.random.fold_in(key_list[1], 1), 0, 1),
        "left_factor": scatter_about(key_list[2], (AW, V, NAUX), (V * max(2, NAUX // 150)) ** -0.5, 0.0390625, ((1, 8), (2, 4))),
        "left_mask": set_ends((jax.random.randint(key_list[3], (NVT, NQT), 0, 2) < 1).astype(jnp.int32), jax.random.fold_in(key_list[3], 1), 0, 1),
        "right_factor": scatter_about(key_list[4], (V, BW, NAUX), (V * max(2, NAUX // 150)) ** -0.5, 0.0390625, ((0, 64), (2, 4))),
        "right_mask": set_ends((jax.random.randint(key_list[5], (NVT, NQT), 0, 2) < 1).astype(jnp.int32), jax.random.fold_in(key_list[5], 1), 0, 1),
        "residual_in": scatter_about(key_list[6], (PAIRS, BW, AW), 1.0, 6.0, ((0, 8),), jnp.float32),
    }


def expand_tiles(mask, width):
    grown = jnp.repeat(jnp.repeat(mask, width, axis=-2), width, axis=-1)
    return grown.astype(jnp.float32)


def reference(amplitudes, pair_mask, left_factor, left_mask, right_factor, right_mask, residual_in):
    left = left_factor.astype(jnp.float32) * expand_tiles(left_mask, TILE)[None, :, :]
    right = right_factor.astype(jnp.float32) * expand_tiles(right_mask, TILE)[:, None, :]
    right_flat = right.reshape(V, BW * NAUX)

    def one_pair(pieces):
        amp, msk = pieces
        tau = amp.astype(jnp.float32) * expand_tiles(msk, TILE)
        inner = jnp.dot(tau, right_flat, precision=lax.Precision.HIGHEST, preferred_element_type=jnp.float32)
        inner = inner.reshape(V, BW, NAUX)
        return jnp.einsum("cbq,acq->ba", inner, left, precision=lax.Precision.HIGHEST)

    ladder = lax.map(one_pair, (amplitudes, pair_mask))
    return residual_in + ladder
```

```python
import functools

import jax
import jax.numpy as jnp
from jax import lax
from jax.experimental import pallas as pl
from jax.experimental.pallas import tpu as pltpu
from jax.sharding import PartitionSpec as P

TILE = 128
NX, NY, NZ = 4, 4, 8
BF, F32 = jnp.bfloat16, jnp.float32
MESH = pl.DeviceIdType.MESH
NT = (((1,), (1,)), ((), ()))


def device(x, y, z, core):
    return {"occ": 2 * x + z // 4, "vir": 2 * (z % 4) + core, "aux": y}


def kernel(
    amp, pmask, left_h, right_h, qmask, out_ref,
    left, rows, rmask, tau, pm, tw, chi, clo, grid_acc, part, got_xy, got_z, mine_z,
    local_sem, ring_send, ring_recv, pair_send, pair_recv,
    tx_send, tx_recv, ty_send, ty_recv, pm_send, pm_recv,
    xy_send, xy_recv, z_send, z_recv,
):
    occ, vir, y = lax.axis_index("occ"), lax.axis_index("vir"), lax.axis_index("aux")
    x, z, core = occ // 2, (occ % 2) * 4 + vir // 2, vir % 2
    here = pl.multiple_of(core * 16, 16)

    local = []
    for block in range(4):
        local.append(pltpu.make_async_copy(
            left_h.at[pl.ds(block * 8, 8)], left.at[pl.ds(block * 8, 8)], local_sem.at[block]))
    own_right = pltpu.make_async_copy(
        right_h, rows.at[:, pl.ds(32 + here, 16), :], local_sem.at[4])
    own_tau = pltpu.make_async_copy(
        amp.at[:, :, pl.ds(pl.multiple_of(x * 256, 256), 256)], tau.at[0], local_sem.at[5])
    own_right.start()
    for copy in local:
        copy.start()
    own_tau.start()
    pm[0] = pmask[x]

    barrier = pltpu.get_barrier_semaphore()
    count = 0
    for dx in range(NX):
        for dy in range(NY):
            if dx or dy:
                pl.semaphore_signal(
                    barrier, inc=1, device_id=device((x + dx) % NX, (y + dy) % NY, z, core),
                    device_id_type=MESH)
                count += 1
    for dz in (1, NZ - 1):
        pl.semaphore_signal(
            barrier, inc=1, device_id=device(x, y, (z + dz) % NZ, core), device_id_type=MESH)
        count += 1
    for dv in range(1, 8):
        pl.semaphore_signal(
            barrier, inc=1, device_id={"occ": occ, "vir": (vir + dv) % 8, "aux": y},
            device_id_type=MESH)
        count += 1
    pl.semaphore_wait(barrier, count)

    sent = []

    def ring(way, step, piece):
        src_i, dst_i = ((1 - step) % 8, (-step) % 8) if way == 0 else (1 + step, step + 2)
        to = (z + 1) % NZ if way == 0 else (z + NZ - 1) % NZ
        return pltpu.make_async_remote_copy(
            src_ref=rows.at[pl.ds(2 * piece, 2), pl.ds(src_i * 32 + here, 16), :],
            dst_ref=rows.at[pl.ds(2 * piece, 2), pl.ds(dst_i * 32 + here, 16), :],
            send_sem=ring_send.at[way, step, piece], recv_sem=ring_recv.at[way, step, piece],
            device_id=device(x, y, to, core), device_id_type=MESH)

    def pair(i):
        return pltpu.make_async_remote_copy(
            src_ref=rows.at[:, pl.ds(i * 32 + here, 16), :],
            dst_ref=rows.at[:, pl.ds(i * 32 + here, 16), :],
            send_sem=pair_send.at[i], recv_sem=pair_recv.at[i],
            device_id=device(x, y, z, 1 - core), device_id_type=MESH)

    def go(copy):
        copy.start()
        sent.append(copy)

    def tau_x(dx, first, size, sem):
        to = (x + dx) % NX
        return pltpu.make_async_remote_copy(
            src_ref=amp.at[pl.ds(first, size), :, pl.ds(pl.multiple_of(to * 256, 256), 256)],
            dst_ref=tau.at[(-dx) % 4, pl.ds(first, size)],
            send_sem=tx_send.at[sem], recv_sem=tx_recv.at[sem],
            device_id=device(to, y, z, core), device_id_type=MESH)

    def tau_y(slot, first, size, dy):
        return pltpu.make_async_remote_copy(
            src_ref=tau.at[slot, pl.ds(first, size)], dst_ref=tau.at[slot, pl.ds(first, size)],
            send_sem=ty_send.at[slot, dy], recv_sem=ty_recv.at[slot, dy],
            device_id=device(x, (y + dy) % NY, z, core), device_id_type=MESH)

    def mask_x(dx):
        to = (x + dx) % NX
        return pltpu.make_async_remote_copy(
            src_ref=pmask.at[to], dst_ref=pm.at[(-dx) % 4],
            send_sem=pm_send.at[dx], recv_sem=pm_recv.at[dx],
            device_id=device(to, y, z, core), device_id_type=MESH)

    split = {1: (4 + y, 1), 2: (2 * y, 2), 3: (4 + y, 1)}
    own_right.wait()
    for piece in range(2):
        for way in range(2):
            go(ring(way, 0, piece))
    go(pair(1))
    x_split = {dx: tau_x(dx, *split[dx], dx) for dx in (2, 1, 3)}
    x_whole = {dx: tau_x(dx, 0, 4, 3 + dx) for dx in (1, 3)}
    masks = {dx: mask_x(dx) for dx in (1, 2, 3)}
    for copy in x_split.values():
        go(copy)
    for copy in masks.values():
        go(copy)
    for copy in x_whole.values():
        go(copy)

    def forward(step, nexts):
        for piece in range(2):
            for way in range(2):
                if (way, piece) not in RECEIVED[step]:
                    continue
                ring(way, step, piece).wait_recv()
                if (way, piece) in nexts:
                    go(ring(way, step + 1, piece))

    both = [(0, 0), (0, 1), (1, 0), (1, 1)]
    RECEIVED = {0: both, 1: both, 2: both, 3: [(0, 0), (1, 1)]}

    forward(0, both)
    go(pair(0))
    go(pair(2))
    y_copies = {}
    for dx in (2, 1, 3):
        x_split[dx].wait_recv()
        slot = (-dx) % 4
        for dy in (2, 1, 3):
            y_copies[slot, dy] = tau_y(slot, *split[dx], dy)
            go(y_copies[slot, dy])
    forward(1, both)
    go(pair(3))
    go(pair(7))

    def mask_rows(half):
        for i in range(4 * half, 4 * half + 4):
            pair(i).wait_recv()
        for i in range(4 * half, 4 * half + 4):
            tile = ((z + i + 7) % NZ) // 4
            row = qmask[pl.ds(tile, 1), :].astype(BF)
            for b in range(4):
                rmask[b * 128 + (i % 4) * 32: b * 128 + (i % 4) * 32 + 32, :] = (
                    rows[b, i * 32: i * 32 + 32, :] * row)

    def couple(half, block):
        lhs = left[block * 8: block * 8 + 8].reshape(8 * 128, 1024)
        prod = lax.dot_general(lhs, rmask[...], NT, preferred_element_type=F32)
        for g in range(16):
            blk = jnp.concatenate(
                [prod[a * 128 + g * 8: a * 128 + g * 8 + 8, :] for a in range(8)], axis=0)
            hi = blk.astype(BF)
            lo = (blk - hi.astype(F32)).astype(BF)
            for b in range(4):
                first = (b * 32 + block * 8) * 8
                chi[g, first: first + 64, half * 128: half * 128 + 128] = hi[:, b * 128: b * 128 + 128]
                clo[g, first: first + 64, half * 128: half * 128 + 128] = lo[:, b * 128: b * 128 + 128]

    for copy in local:
        copy.wait()
    mask_rows(0)
    couple(0, 0)
    couple(0, 1)
    forward(2, [(0, 0), (1, 1)])
    go(pair(6))
    go(pair(4))
    couple(0, 2)
    forward(3, [])
    go(pair(5))
    couple(0, 3)

    own_tau.wait()
    for dx in (1, 3):
        x_whole[dx].wait_recv()
    for dx in (1, 2, 3):
        masks[dx].wait_recv()
    for slot in (2, 3, 1):
        for dy in (1, 2, 3):
            y_copies[slot, dy].wait_recv()
    shift = ((9 - z) % 8) * 32

    def turn(step, _):
        slot, p = step // 4, (step % 4) * 2
        parts = []
        for k in range(2):
            block = tau[slot, p + k].astype(F32) * pm[slot, pl.ds(p + k, 1), :]
            parts.append(pltpu.roll(block, shift, 1))
        for g in range(16):
            pack = jnp.concatenate([v[g * 8: g * 8 + 8, :] for v in parts], axis=0)
            tw[g, pl.ds(pl.multiple_of(step * 16, 16), 16), :] = pack.astype(BF)
        return 0

    lax.fori_loop(0, 16, turn, 0)

    mask_rows(1)
    for block in range(4):
        couple(1, block)

    grid_acc[...] = jnp.zeros_like(grid_acc)

    def contract(step, _):
        total = grid_acc[...]
        for k in range(4):
            g = step * 4 + k
            total = total + lax.dot_general(chi[g], tw[g], NT, preferred_element_type=F32)
            total = total + lax.dot_general(clo[g], tw[g], NT, preferred_element_type=F32)
        grid_acc[...] = total
        return 0

    lax.fori_loop(0, 4, contract, 0)

    acc = grid_acc[...].reshape(128, 8, 256)
    same = (lax.broadcasted_iota(jnp.int32, (128, 8, 256), 2) % 8
            == lax.broadcasted_iota(jnp.int32, (128, 8, 256), 1))
    diag = jnp.where(same, acc, 0.0).sum(axis=1)
    pick = (lax.broadcasted_iota(jnp.int32, (32, 256), 1) // 8
            == lax.broadcasted_iota(jnp.int32, (32, 256), 0)).astype(F32).astype(BF)
    ladder = jnp.zeros((32, 128), F32)
    rest = diag
    for _ in range(3):
        top = rest.astype(BF)
        rest = rest - top.astype(F32)
        ladder = ladder + lax.dot_general(pick, top, NT, preferred_element_type=F32)
    part[...] = ladder.reshape(4, 8, 128)

    index = x * 4 + y
    got_xy[index] = part[0]

    def to_xy(dx, dy):
        return pltpu.make_async_remote_copy(
            src_ref=part.at[dx], dst_ref=got_xy.at[index],
            send_sem=xy_send.at[dx * 4 + dy], recv_sem=xy_recv.at[dx * 4 + dy],
            device_id=device((x + dx) % NX, (y + dy) % NY, z, core), device_id_type=MESH)

    pairs = [(dx, dy) for dx in range(4) for dy in range(4) if dx or dy]
    xy = [to_xy(dx, dy) for dx, dy in sorted(pairs, key=lambda d: -(d[0] == 2) - (d[1] == 2))]
    for copy in xy:
        go(copy)
    for copy in xy:
        copy.wait_recv()
    total = got_xy[0]
    for k in range(1, 16):
        total = total + got_xy[k]
    mine_z[...] = total
    got_z[vir] = total

    def to_z(dv):
        return pltpu.make_async_remote_copy(
            src_ref=mine_z, dst_ref=got_z.at[vir],
            send_sem=z_send.at[dv], recv_sem=z_recv.at[dv],
            device_id={"occ": occ, "vir": (vir + dv) % 8, "aux": y}, device_id_type=MESH)

    zs = [to_z(dv) for dv in range(1, 8)]
    for copy in zs:
        go(copy)
    for copy in zs:
        copy.wait_recv()
    total = got_z[0]
    for k in range(1, 8):
        total = total + got_z[k]
    out_ref[...] = total
    for copy in sent:
        copy.wait_send()


def local(amplitudes, pair_mask, left_factor, left_mask, right_factor, right_mask, residual_in):
    x = lax.axis_index("occ") // 2
    pmask = jnp.repeat(
        pair_mask.reshape(8, 4, 2).transpose(1, 0, 2).astype(F32), TILE, axis=2)
    tiles = lax.dynamic_slice_in_dim(right_mask, 2 * x, 2, axis=0) * left_mask
    qmask = jnp.repeat(tiles.astype(F32), TILE, axis=1)
    right_t = right_factor.transpose(1, 0, 2)
    dma = pltpu.SemaphoreType.DMA
    vmem = pltpu.VMEM
    any_spec = pl.BlockSpec(memory_space=pl.ANY)
    vmem_spec = pl.BlockSpec(memory_space=pltpu.VMEM)
    ladder = pl.pallas_call(
        kernel,
        out_shape=jax.ShapeDtypeStruct((8, 128), F32),
        in_specs=[any_spec, vmem_spec, any_spec, any_spec, vmem_spec],
        out_specs=vmem_spec,
        scratch_shapes=[
            vmem((32, 128, 1024), BF),
            vmem((4, 256, 1024), BF),
            vmem((512, 1024), BF),
            vmem((4, 8, 128, 256), BF),
            vmem((4, 8, 256), F32),
            vmem((16, 256, 256), BF),
            vmem((16, 1024, 256), BF),
            vmem((16, 1024, 256), BF),
            vmem((1024, 256), F32),
            vmem((4, 8, 128), F32),
            vmem((16, 8, 128), F32),
            vmem((8, 8, 128), F32),
            vmem((8, 128), F32),
            dma((6,)),
            dma((2, 4, 2)), dma((2, 4, 2)),
            dma((8,)), dma((8,)),
            dma((7,)), dma((7,)),
            dma((4, 4)), dma((4, 4)),
            dma((4,)), dma((4,)),
            dma((16,)), dma((16,)),
            dma((8,)), dma((8,)),
        ],
        compiler_params=pltpu.CompilerParams(
            collective_id=0, has_side_effects=True, vmem_limit_bytes=62 * 1024 * 1024),
        name="ladder",
    )(amplitudes, pmask, left_factor, right_t, qmask)
    return residual_in + ladder.reshape(residual_in.shape)


def solution(mesh):
    return jax.shard_map(
        local,
        mesh=mesh,
        in_specs=(
            P("occ", "vir", None),
            P("occ", "vir", None),
            P(None, "vir", "aux"),
            P("vir", "aux"),
            P(("occ", "vir"), None, "aux"),
            P(None, "aux"),
            P("occ", None, None),
        ),
        out_specs=P("occ", None, None),
        check_vma=False,
    )
```

```python
import jax
import jax.numpy as jnp
from jax import lax
from jax.experimental import pallas as pl
from jax.experimental.pallas import tpu as pltpu
from jax.sharding import PartitionSpec as P

NX, NY, NZ = 4, 4, 8
BF, F32 = jnp.bfloat16, jnp.float32
MESH = pl.DeviceIdType.MESH
NT = (((1,), (1,)), ((), ()))


def mod(value, n):
    return lax.rem(value, n)


def device(x, y, z, core):
    return {"occ": 2 * x + lax.div(z, 4), "vir": 2 * mod(z, 4) + core, "aux": y}


def kernel(
    amp, pmask_h, left_h, lmask_h, right_h, rmask_h, out_ref,
    left, raw, rows, rside, tau0, tau1, tau2, tau3, pmask_v, lmask_v, rmask_v, qm, pmx, pm, tw, parts,
    grid_acc, part, got_xy, got_z, mine_z,
    local_sem, ring_send, ring_recv, pair_send, pair_recv,
    tx_send, tx_recv, ty_send, ty_recv, pm_send, pm_recv,
    xy_send, xy_recv, z_send, z_recv,
):
    occ, vir, y = lax.axis_index("occ"), lax.axis_index("vir"), lax.axis_index("aux")
    x, z, core = lax.div(occ, 2), mod(occ, 2) * 4 + lax.div(vir, 2), mod(vir, 2)
    here = pl.multiple_of(core * 16, 16)
    mine = pl.ds(pl.multiple_of(x * 256, 256), 256)

    tau = (tau0, tau1, tau2, tau3)

    own_right = pltpu.make_async_copy(right_h, raw, local_sem.at[4])
    own_tau = pltpu.make_async_copy(amp.at[:, :, mine], tau0, local_sem.at[5])
    small = [
        pltpu.make_async_copy(pmask_h, pmask_v, local_sem.at[6]),
        pltpu.make_async_copy(lmask_h, lmask_v, local_sem.at[7]),
        pltpu.make_async_copy(rmask_h, rmask_v, local_sem.at[8]),
    ]
    loads = [
        pltpu.make_async_copy(
            left_h.at[pl.ds(k * 8, 8)], left.at[pl.ds(k * 8, 8)], local_sem.at[k])
        for k in range(4)
    ]
    own_right.start()
    for copy in small:
        copy.start()
    for copy in loads:
        copy.start()
    own_tau.start()

    barrier = pltpu.get_barrier_semaphore()
    others = [device(mod(x + dx, NX), mod(y + dy, NY), z, core)
              for dx in range(NX) for dy in range(NY) if dx or dy]
    others += [device(x, y, mod(z + dz, NZ), core) for dz in (1, NZ - 1)]
    others += [{"occ": occ, "vir": mod(vir + dv, 8), "aux": y} for dv in range(1, 8)]
    for other in others:
        pl.semaphore_signal(barrier, inc=1, device_id=other, device_id_type=MESH)

    own_right.wait()
    wide = raw[...].astype(F32)
    for b in range(4):
        rows[b, pl.ds(32 + here, 16), :] = wide[:, b, :].astype(BF)
    for copy in small:
        copy.wait()
    tiles = (rmask_v[...] * lmask_v[...]).astype(F32)
    for q in range(8):
        qm[:, q * 128: q * 128 + 128] = jnp.broadcast_to(tiles[:, q: q + 1], (8, 128))
    ptile = pmask_v[...].reshape(8, 8).astype(F32)
    for t in range(8):
        pmx[t // 2, :, (t % 2) * 128: (t % 2) * 128 + 128] = jnp.broadcast_to(
            ptile[:, t: t + 1], (8, 128))
    pl.semaphore_wait(barrier, len(others))

    sent = []

    def go(copy):
        copy.start()
        sent.append(copy)

    def ring(way, step, b):
        src_i, dst_i = ((1 - step) % 8, (-step) % 8) if way == 0 else (1 + step, step + 2)
        to = mod(z + 1, NZ) if way == 0 else mod(z + NZ - 1, NZ)
        return pltpu.make_async_remote_copy(
            src_ref=rows.at[b, pl.ds(src_i * 32 + here, 16), :],
            dst_ref=rows.at[b, pl.ds(dst_i * 32 + here, 16), :],
            send_sem=ring_send.at[way, step, b], recv_sem=ring_recv.at[way, step, b],
            device_id=device(x, y, to, core), device_id_type=MESH)

    def pair(i):
        return pltpu.make_async_remote_copy(
            src_ref=rows.at[:, pl.ds(i * 32 + here, 16), :],
            dst_ref=rows.at[:, pl.ds(i * 32 + here, 16), :],
            send_sem=pair_send.at[i], recv_sem=pair_recv.at[i],
            device_id=device(x, y, z, 1 - core), device_id_type=MESH)

    def tau_x(dx, first, size):
        to = mod(x + dx, NX)
        return pltpu.make_async_remote_copy(
            src_ref=amp.at[pl.ds(first, size), :, pl.ds(pl.multiple_of(to * 256, 256), 256)],
            dst_ref=tau[(-dx) % 4].at[pl.ds(first, size)],
            send_sem=tx_send.at[dx], recv_sem=tx_recv.at[dx],
            device_id=device(to, y, z, core), device_id_type=MESH)

    def tau_y(dy):
        return pltpu.make_async_remote_copy(
            src_ref=tau2.at[pl.ds(2 * y, 2)], dst_ref=tau2.at[pl.ds(2 * y, 2)],
            send_sem=ty_send.at[dy], recv_sem=ty_recv.at[dy],
            device_id=device(x, mod(y + dy, NY), z, core), device_id_type=MESH)

    def mask_x(dx):
        to = mod(x + dx, NX)
        return pltpu.make_async_remote_copy(
            src_ref=pmx.at[to], dst_ref=pm.at[(-dx) % 4],
            send_sem=pm_send.at[dx], recv_sem=pm_recv.at[dx],
            device_id=device(to, y, z, core), device_id_type=MESH)

    x_copies = {1: tau_x(1, 0, 8), 2: tau_x(2, 2 * y, 2), 3: tau_x(3, 0, 8)}
    y_copies = {dy: tau_y(dy) for dy in (1, 2, 3)}
    masks = {dx: mask_x(dx) for dx in (1, 2, 3)}

    firsts = [[ring(way, 0, b) for way in (0, 1)] for b in range(4)]
    for b in range(4):
        for copy in firsts[b]:
            go(copy)
        if b == 0:
            go(pair(1))

    def arrived(way, step, b):
        ring(way, step, b).wait_recv()
        if step < 2 or (step == 2 and (b < 2) == (way == 0)):
            go(ring(way, step + 1, b))

    def stage(step, b):
        for way in (0, 1):
            if step < 3 or (b < 2) == (way == 0):
                arrived(way, step, b)

    def across(*chips):
        for i in chips:
            go(pair(i))

    def turn(slot):
        shift = mod(9 - z, 8) * 32

        def two(step, _):
            parts = []
            for k in range(2):
                p = step * 2 + k
                mask = (pmx[x, pl.ds(p, 1), :] if slot == 0 else pm[slot, pl.ds(p, 1), :])
                parts.append(pltpu.roll(tau[slot][p].astype(F32) * mask, shift, 1))
            first = pl.multiple_of(slot * 64 + step * 16, 16)
            for odd in range(2):
                if odd:
                    parts = [jnp.concatenate(
                        [pltpu.roll(v[:, h * 128: h * 128 + 128], 64, 1) for h in range(2)],
                        axis=1) for v in parts]
                for g in range(16):
                    both = jnp.concatenate([v[g * 8: g * 8 + 8, :] for v in parts], axis=0)
                    tw[odd, g, pl.ds(first, 16), :] = both.astype(BF)
            return 0

        lax.fori_loop(0, 4, two, 0)

    CHUNKS = {0: (0, 0, 0), 1: (2, 0, 1), 2: (6, 1, 1), 3: (4, 1, 0)}

    def gather(m):
        first, h, place = CHUNKS[m]
        for i in (first, first + 1):
            pair(i).wait_recv()
        for i in (first, first + 1):
            row = qm[pl.ds(2 * x + lax.div(mod(z + i + 7, NZ), 4), 1), :].astype(BF)
            for b in range(4):
                at = (b ^ place) * 64 + (i - first) * 32
                rside[at: at + 32, :] = rows[b, i * 32: i * 32 + 32, :] * row

    def couple(m, block):
        first, h, place = CHUNKS[m]
        lhs = left[pl.ds(block * 8, 8)].reshape(8 * 128, 1024)
        prod = lax.dot_general(lhs, rside[...], NT, preferred_element_type=F32)
        for g in range(16):
            blk = jnp.concatenate(
                [prod[a * 128 + g * 8: a * 128 + g * 8 + 8, :] for a in range(8)], axis=0)
            hi = blk.astype(BF)
            lo = (blk - hi.astype(F32)).astype(BF)
            for at in range(4):
                b = at ^ place
                lane = h * 128 + (at % 2) * 64
                for low, value in ((0, hi), (512, lo)):
                    top = pl.multiple_of(low + (b // 2) * 256 + block * 64, 64)
                    parts[g, b % 2, pl.ds(top, 64), lane: lane + 64] = (
                        value[:, at * 64: at * 64 + 64])

    def chunk(m):
        gather(m)
        lax.fori_loop(0, 4, lambda k, c: couple(m, k) or c, 0)

    def passed(step):
        for b in range(4):
            stage(step, b)

    for copy in loads:
        copy.wait()
    passed(0)
    across(0, 2)
    for dx in (2, 1, 3):
        go(x_copies[dx])
    for copy in masks.values():
        go(copy)
    chunk(0)
    x_copies[2].wait_recv()
    for dy in (2, 1, 3):
        go(y_copies[dy])
    passed(1)
    across(3, 7)
    own_tau.wait()
    turn(0)
    chunk(1)
    passed(2)
    across(4, 6)
    for dx in (1, 2, 3):
        masks[dx].wait_recv()
    for dy in (1, 2, 3):
        y_copies[dy].wait_recv()
    turn(2)
    chunk(2)
    passed(3)
    across(5)
    x_copies[3].wait_recv()
    turn(1)
    x_copies[1].wait_recv()
    turn(3)
    chunk(3)

    grid_acc[...] = jnp.zeros_like(grid_acc)

    def contract(step, _):
        for odd in range(2):
            total = jnp.zeros((1024, 256), F32)
            for k in range(4):
                g = step * 4 + k
                total = total + lax.dot_general(
                    parts[g, odd], tw[odd, g], NT, preferred_element_type=F32)
            grid_acc[odd * 512: odd * 512 + 512, :] += total[:512] + total[512:]
        return 0

    lax.fori_loop(0, 4, contract, 0)

    acc = grid_acc[...].reshape(128, 8, 256)
    same = (lax.broadcasted_iota(jnp.int32, (128, 8, 256), 2) % 8
            == lax.broadcasted_iota(jnp.int32, (128, 8, 256), 1))
    diag = jnp.where(same, acc, 0.0).sum(axis=1)
    pick = (lax.broadcasted_iota(jnp.int32, (32, 256), 1) // 8
            == lax.broadcasted_iota(jnp.int32, (32, 256), 0)).astype(F32).astype(BF)
    ladder = jnp.zeros((32, 128), F32)
    rest = diag
    for _ in range(3):
        top = rest.astype(BF)
        rest = rest - top.astype(F32)
        ladder = ladder + lax.dot_general(pick, top, NT, preferred_element_type=F32)
    part[...] = ladder.reshape(4, 8, 128)

    index = x * 4 + y
    got_xy[index] = part[0]

    def to_xy(dx, dy):
        return pltpu.make_async_remote_copy(
            src_ref=part.at[dx], dst_ref=got_xy.at[index],
            send_sem=xy_send.at[dx * 4 + dy], recv_sem=xy_recv.at[dx * 4 + dy],
            device_id=device(mod(x + dx, NX), mod(y + dy, NY), z, core), device_id_type=MESH)

    total = part[0]
    pairs = [(dx, dy) for dx in range(4) for dy in range(4) if dx or dy]
    xy = [to_xy(dx, dy) for dx, dy in sorted(pairs, key=lambda d: -(d[0] == 2) - (d[1] == 2))]
    for copy in xy:
        go(copy)
    for copy in xy:
        copy.wait_recv()
    total = got_xy[0]
    for k in range(1, 16):
        total = total + got_xy[k]
    mine_z[...] = total
    got_z[vir] = total

    def to_z(dv):
        return pltpu.make_async_remote_copy(
            src_ref=mine_z, dst_ref=got_z.at[vir],
            send_sem=z_send.at[dv], recv_sem=z_recv.at[dv],
            device_id={"occ": occ, "vir": mod(vir + dv, 8), "aux": y}, device_id_type=MESH)

    zs = [to_z(dv) for dv in range(1, 8)]
    for copy in zs:
        go(copy)
    for copy in zs:
        copy.wait_recv()
    total = got_z[0]
    for k in range(1, 8):
        total = total + got_z[k]
    for at, b in enumerate((0, 2, 1, 3)):
        out_ref[pl.ds(b, 8, stride=4), :] = total[:, at * 32: at * 32 + 32]
    for copy in sent:
        copy.wait_send()


def local(amplitudes, pair_mask, left_factor, left_mask, right_factor, right_mask, residual_in):
    dma = pltpu.SemaphoreType.DMA
    vmem = pltpu.VMEM
    ladder = pl.pallas_call(
        kernel,
        out_shape=jax.ShapeDtypeStruct((32, 32), F32),
        in_specs=[pl.BlockSpec(memory_space=pl.ANY)] * 6,
        out_specs=pl.BlockSpec(memory_space=pltpu.VMEM),
        scratch_shapes=[
            vmem((32, 128, 1024), BF),
            vmem((16, 4, 1024), BF),
            vmem((4, 256, 1024), BF),
            vmem((256, 1024), BF),
            vmem((8, 128, 256), BF), vmem((8, 128, 256), BF),
            vmem((8, 128, 256), BF), vmem((8, 128, 256), BF),
            vmem((8, 1, 8), jnp.int32),
            vmem((1, 8), jnp.int32),
            vmem((8, 8), jnp.int32),
            vmem((8, 1024), F32),
            vmem((4, 8, 256), F32),
            vmem((4, 8, 256), F32),
            vmem((2, 16, 256, 256), BF),
            vmem((16, 2, 1024, 256), BF),
            vmem((1024, 256), F32),
            vmem((4, 8, 128), F32),
            vmem((16, 8, 128), F32),
            vmem((8, 8, 128), F32),
            vmem((8, 128), F32),
            dma((9,)),
            dma((2, 4, 4)), dma((2, 4, 4)),
            dma((8,)), dma((8,)),
            dma((4,)), dma((4,)),
            dma((4,)), dma((4,)),
            dma((4,)), dma((4,)),
            dma((16,)), dma((16,)),
            dma((8,)), dma((8,)),
        ],
        compiler_params=pltpu.CompilerParams(
            collective_id=0, has_side_effects=True, vmem_limit_bytes=62 * 1024 * 1024),
        name="ladder",
    )(amplitudes, pair_mask, left_factor, left_mask, right_factor, right_mask)
    return residual_in + ladder.reshape(residual_in.shape)


def solution(mesh):
    return jax.shard_map(
        local,
        mesh=mesh,
        in_specs=(
            P("occ", "vir", None),
            P("occ", "vir", None),
            P(None, "vir", "aux"),
            P("vir", "aux"),
            P(("occ", "vir"), None, "aux"),
            P(None, "aux"),
            P("occ", None, None),
        ),
        out_specs=P("occ", None, None),
        check_vma=False,
    )
```

```python
import jax
import jax.numpy as jnp
from jax import lax
from jax.experimental import pallas as pl
from jax.experimental.pallas import tpu as pltpu
from jax.sharding import PartitionSpec as P

NX, NY, NZ = 4, 4, 8
BF, F32 = jnp.bfloat16, jnp.float32
MESH = pl.DeviceIdType.MESH
NT = (((1,), (1,)), ((), ()))


def mod(value, n):
    return lax.rem(value, n)


def device(x, y, z, core):
    return {"occ": 2 * x + lax.div(z, 4), "vir": 2 * mod(z, 4) + core, "aux": y}


def kernel(
    amp, pmask_h, left_h, lmask_h, right_h, rmask_h, out_ref,
    left, raw, rows, rside, tau0, tau1, tau2, tau3, pmask_v, lmask_v, rmask_v, qm, pmx, pm, tw, parts,
    grid_acc, part, got_xy, got_z, mine_z,
    local_sem, ring_send, ring_recv, pair_send, pair_recv,
    tx_send, tx_recv, ty_send, ty_recv, pm_send, pm_recv,
    xy_send, xy_recv, z_send, z_recv,
):
    occ, vir, y = lax.axis_index("occ"), lax.axis_index("vir"), lax.axis_index("aux")
    x, z, core = lax.div(occ, 2), mod(occ, 2) * 4 + lax.div(vir, 2), mod(vir, 2)
    here = pl.multiple_of(core * 16, 16)
    mine = pl.ds(pl.multiple_of(x * 256, 256), 256)

    tau = (tau0, tau1, tau2, tau3)

    own_right = pltpu.make_async_copy(right_h, raw, local_sem.at[4])
    own_tau = pltpu.make_async_copy(amp.at[:, :, mine], tau0, local_sem.at[5])
    small = [
        pltpu.make_async_copy(pmask_h, pmask_v, local_sem.at[6]),
        pltpu.make_async_copy(lmask_h, lmask_v, local_sem.at[7]),
        pltpu.make_async_copy(rmask_h, rmask_v, local_sem.at[8]),
    ]
    loads = [
        pltpu.make_async_copy(
            left_h.at[pl.ds(k * 8, 8)], left.at[pl.ds(k * 8, 8)], local_sem.at[k])
        for k in range(4)
    ]
    own_right.start()
    for copy in small:
        copy.start()
    for copy in loads:
        copy.start()
    own_tau.start()

    barrier = pltpu.get_barrier_semaphore()
    others = [device(mod(x + dx, NX), mod(y + dy, NY), z, core)
              for dx in range(NX) for dy in range(NY) if dx or dy]
    others += [device(x, y, mod(z + dz, NZ), core) for dz in (1, NZ - 1)]
    others += [{"occ": occ, "vir": mod(vir + dv, 8), "aux": y} for dv in range(1, 8)]
    for other in others:
        pl.semaphore_signal(barrier, inc=1, device_id=other, device_id_type=MESH)

    own_right.wait()
    wide = raw[...].astype(F32)
    for b in range(4):
        rows[b, pl.ds(32 + here, 16), :] = wide[:, b, :].astype(BF)
    for copy in small:
        copy.wait()
    tiles = (rmask_v[...] * lmask_v[...]).astype(F32)
    for q in range(8):
        qm[:, q * 128: q * 128 + 128] = jnp.broadcast_to(tiles[:, q: q + 1], (8, 128))
    ptile = pmask_v[...].reshape(8, 8).astype(F32)
    for t in range(8):
        pmx[t // 2, :, (t % 2) * 128: (t % 2) * 128 + 128] = jnp.broadcast_to(
            ptile[:, t: t + 1], (8, 128))
    pl.semaphore_wait(barrier, len(others))

    sent = []

    def go(make, *args):
        make(*args).start()
        sent.append((make, args))

    def ring(way, step, b):
        src_i, dst_i = ((1 - step) % 8, (-step) % 8) if way == 0 else (1 + step, step + 2)
        to = mod(z + 1, NZ) if way == 0 else mod(z + NZ - 1, NZ)
        return pltpu.make_async_remote_copy(
            src_ref=rows.at[b, pl.ds(src_i * 32 + here, 16), :],
            dst_ref=rows.at[b, pl.ds(dst_i * 32 + here, 16), :],
            send_sem=ring_send.at[way, step, b], recv_sem=ring_recv.at[way, step, b],
            device_id=device(x, y, to, core), device_id_type=MESH)

    def pair(i):
        return pltpu.make_async_remote_copy(
            src_ref=rows.at[:, pl.ds(i * 32 + here, 16), :],
            dst_ref=rows.at[:, pl.ds(i * 32 + here, 16), :],
            send_sem=pair_send.at[i], recv_sem=pair_recv.at[i],
            device_id=device(x, y, z, 1 - core), device_id_type=MESH)

    def tau_x(dx, first, size):
        to = mod(x + dx, NX)
        return pltpu.make_async_remote_copy(
            src_ref=amp.at[pl.ds(first, size), :, pl.ds(pl.multiple_of(to * 256, 256), 256)],
            dst_ref=tau[(-dx) % 4].at[pl.ds(first, size)],
            send_sem=tx_send.at[dx], recv_sem=tx_recv.at[dx],
            device_id=device(to, y, z, core), device_id_type=MESH)

    def tau_y(dy):
        return pltpu.make_async_remote_copy(
            src_ref=tau2.at[pl.ds(2 * y, 2)], dst_ref=tau2.at[pl.ds(2 * y, 2)],
            send_sem=ty_send.at[dy], recv_sem=ty_recv.at[dy],
            device_id=device(x, mod(y + dy, NY), z, core), device_id_type=MESH)

    def mask_x(dx):
        to = mod(x + dx, NX)
        return pltpu.make_async_remote_copy(
            src_ref=pmx.at[to], dst_ref=pm.at[(-dx) % 4],
            send_sem=pm_send.at[dx], recv_sem=pm_recv.at[dx],
            device_id=device(to, y, z, core), device_id_type=MESH)

    SPAN = {1: (0, 8), 2: (2 * y, 2), 3: (0, 8)}
    for b in range(4):
        for way in (0, 1):
            go(ring, way, 0, b)
        if b == 0:
            go(pair, 1)
    for dx in (1, 2, 3):
        go(mask_x, dx)
    go(tau_x, 2, *SPAN[2])

    def arrived(way, step, b):
        ring(way, step, b).wait_recv()
        if step < 2 or (step == 2 and (b < 2) == (way == 0)):
            go(ring, way, step + 1, b)

    def passed(step):
        for b in range(4):
            for way in (0, 1):
                if step < 3 or (b < 2) == (way == 0):
                    arrived(way, step, b)

    def across(*chips):
        for i in chips:
            go(pair, i)

    def turn(slot):
        shift = mod(9 - z, 8) * 32

        def two(step, _):
            parts = []
            for k in range(2):
                p = step * 2 + k
                mask = (pmx[x, pl.ds(p, 1), :] if slot == 0 else pm[slot, pl.ds(p, 1), :])
                parts.append(pltpu.roll(tau[slot][p].astype(F32) * mask, shift, 1))
            first = pl.multiple_of(slot * 64 + step * 16, 16)
            for odd in range(2):
                if odd:
                    parts = [jnp.concatenate(
                        [pltpu.roll(v[:, h * 128: h * 128 + 128], 64, 1) for h in range(2)],
                        axis=1) for v in parts]
                for g in range(16):
                    both = jnp.concatenate([v[g * 8: g * 8 + 8, :] for v in parts], axis=0)
                    tw[odd, g, pl.ds(first, 16), :] = both.astype(BF)
            return 0

        lax.fori_loop(0, 4, two, 0)

    def gather(m, first, place):
        for k in range(2):
            pair(first + k).wait_recv()
        for k in range(2):
            i = first + k
            row = qm[pl.ds(2 * x + lax.div(mod(z + i + 7, NZ), 4), 1), :].astype(BF)
            from_row = pl.multiple_of(i * 32, 32)
            for at in range(4):
                b = (at // 2) * 2 + mod(at + place, 2)
                rside[at * 64 + k * 32: at * 64 + k * 32 + 32, :] = (
                    rows[b, pl.ds(from_row, 32), :] * row)

    def couple(h, place, block):
        lhs = left[pl.ds(block * 8, 8)].reshape(8 * 128, 1024)
        prod = lax.dot_general(lhs, rside[...], NT, preferred_element_type=F32)
        for g in range(16):
            blk = jnp.concatenate(
                [prod[a * 128 + g * 8: a * 128 + g * 8 + 8, :] for a in range(8)], axis=0)
            hi = blk.astype(BF)
            lo = (blk - hi.astype(F32)).astype(BF)
            for at in range(4):
                lane = (at % 2) * 64
                for low, value in ((0, hi), (512, lo)):
                    top = pl.multiple_of(low + (at // 2) * 256 + block * 64, 64)
                    parts[h, g, mod(at + place, 2), pl.ds(top, 64), lane: lane + 64] = (
                        value[:, at * 64: at * 64 + 64])

    own_tau.wait()
    turn(0)
    for copy in loads:
        copy.wait()
    passed(0)
    across(0, 2)
    go(tau_x, 1, *SPAN[1])
    go(tau_x, 3, *SPAN[3])
    tau_x(2, *SPAN[2]).wait_recv()
    for dy in (2, 1, 3):
        go(tau_y, dy)

    def chunk(m, _):
        h = lax.div(m, 2)
        place = mod(h + m, 2)
        gather(m, 2 * m + h * (10 - 4 * m), place)

        def two(k, _):
            couple(h, place, 2 * k)
            couple(h, place, 2 * k + 1)
            return 0

        lax.fori_loop(0, 2, two, 0)

        @pl.when(m == 0)
        def _():
            passed(1)
            across(3, 7)

        @pl.when(m == 1)
        def _():
            passed(2)
            across(4, 6)
            for dx in (1, 2, 3):
                mask_x(dx).wait_recv()
            for dy in (1, 2, 3):
                tau_y(dy).wait_recv()
            turn(2)

        @pl.when(m == 2)
        def _():
            passed(3)
            across(5)
            tau_x(3, *SPAN[3]).wait_recv()
            turn(1)
            tau_x(1, *SPAN[1]).wait_recv()
            turn(3)

        return 0

    lax.fori_loop(0, 4, chunk, 0)

    grid_acc[...] = jnp.zeros_like(grid_acc)

    def contract(step, _):
        for odd in range(2):
            total = jnp.zeros((1024, 256), F32)
            for k in range(4):
                g = step * 4 + k
                both = jnp.concatenate([parts[0, g, odd], parts[1, g, odd]], axis=1)
                total = total + lax.dot_general(
                    both, tw[odd, g], NT, preferred_element_type=F32)
            grid_acc[odd * 512: odd * 512 + 512, :] += total[:512] + total[512:]
        return 0

    lax.fori_loop(0, 4, contract, 0)

    acc = grid_acc[...].reshape(128, 8, 256)
    same = (lax.broadcasted_iota(jnp.int32, (128, 8, 256), 2) % 8
            == lax.broadcasted_iota(jnp.int32, (128, 8, 256), 1))
    diag = jnp.where(same, acc, 0.0).sum(axis=1)
    pick = (lax.broadcasted_iota(jnp.int32, (32, 256), 1) // 8
            == lax.broadcasted_iota(jnp.int32, (32, 256), 0)).astype(F32).astype(BF)
    ladder = jnp.zeros((32, 128), F32)
    rest = diag
    for _ in range(3):
        top = rest.astype(BF)
        rest = rest - top.astype(F32)
        ladder = ladder + lax.dot_general(pick, top, NT, preferred_element_type=F32)
    part[...] = ladder.reshape(4, 8, 128)

    index = x * 4 + y
    got_xy[index] = part[0]

    def to_xy(dx, dy):
        return pltpu.make_async_remote_copy(
            src_ref=part.at[dx], dst_ref=got_xy.at[index],
            send_sem=xy_send.at[dx * 4 + dy], recv_sem=xy_recv.at[dx * 4 + dy],
            device_id=device(mod(x + dx, NX), mod(y + dy, NY), z, core), device_id_type=MESH)

    total = part[0]
    pairs = [(dx, dy) for dx in range(4) for dy in range(4) if dx or dy]
    pairs.sort(key=lambda d: -(d[0] == 2) - (d[1] == 2))
    for dx, dy in pairs:
        go(to_xy, dx, dy)
    for dx, dy in pairs:
        to_xy(dx, dy).wait_recv()
    total = got_xy[0]
    for k in range(1, 16):
        total = total + got_xy[k]
    mine_z[...] = total
    got_z[vir] = total

    def to_z(dv):
        return pltpu.make_async_remote_copy(
            src_ref=mine_z, dst_ref=got_z.at[vir],
            send_sem=z_send.at[dv], recv_sem=z_recv.at[dv],
            device_id={"occ": occ, "vir": mod(vir + dv, 8), "aux": y}, device_id_type=MESH)

    for dv in range(1, 8):
        go(to_z, dv)
    for dv in range(1, 8):
        to_z(dv).wait_recv()
    total = got_z[0]
    for k in range(1, 8):
        total = total + got_z[k]
    for at, b in enumerate((0, 2, 1, 3)):
        out_ref[pl.ds(b, 8, stride=4), :] = total[:, at * 32: at * 32 + 32]
    for make, args in sent:
        make(*args).wait_send()


def local(amplitudes, pair_mask, left_factor, left_mask, right_factor, right_mask, residual_in):
    dma = pltpu.SemaphoreType.DMA
    vmem = pltpu.VMEM
    ladder = pl.pallas_call(
        kernel,
        out_shape=jax.ShapeDtypeStruct((32, 32), F32),
        in_specs=[pl.BlockSpec(memory_space=pl.ANY)] * 6,
        out_specs=pl.BlockSpec(memory_space=pltpu.VMEM),
        scratch_shapes=[
            vmem((32, 128, 1024), BF),
            vmem((16, 4, 1024), BF),
            vmem((4, 256, 1024), BF),
            vmem((256, 1024), BF),
            vmem((8, 128, 256), BF), vmem((8, 128, 256), BF),
            vmem((8, 128, 256), BF), vmem((8, 128, 256), BF),
            vmem((8, 1, 8), jnp.int32),
            vmem((1, 8), jnp.int32),
            vmem((8, 8), jnp.int32),
            vmem((8, 1024), F32),
            vmem((4, 8, 256), F32),
            vmem((4, 8, 256), F32),
            vmem((2, 16, 256, 256), BF),
            vmem((2, 16, 2, 1024, 128), BF),
            vmem((1024, 256), F32),
            vmem((4, 8, 128), F32),
            vmem((16, 8, 128), F32),
            vmem((8, 8, 128), F32),
            vmem((8, 128), F32),
            dma((9,)),
            dma((2, 4, 4)), dma((2, 4, 4)),
            dma((8,)), dma((8,)),
            dma((4,)), dma((4,)),
            dma((4,)), dma((4,)),
            dma((4,)), dma((4,)),
            dma((16,)), dma((16,)),
            dma((8,)), dma((8,)),
        ],
        compiler_params=pltpu.CompilerParams(
            collective_id=0, has_side_effects=True, vmem_limit_bytes=62 * 1024 * 1024),
        name="ladder",
    )(amplitudes, pair_mask, left_factor, left_mask, right_factor, right_mask)
    return residual_in + ladder.reshape(residual_in.shape)


def solution(mesh):
    return jax.shard_map(
        local,
        mesh=mesh,
        in_specs=(
            P("occ", "vir", None),
            P("occ", "vir", None),
            P(None, "vir", "aux"),
            P("vir", "aux"),
            P(("occ", "vir"), None, "aux"),
            P(None, "aux"),
            P("occ", None, None),
        ),
        out_specs=P("occ", None, None),
        check_vma=False,
    )
```

```python
import jax
import jax.numpy as jnp
from jax import lax
from jax.experimental import pallas as pl
from jax.experimental.pallas import tpu as pltpu
from jax.sharding import PartitionSpec as P

NX, NY, NZ = 4, 4, 8
BF, F32 = jnp.bfloat16, jnp.float32
MESH = pl.DeviceIdType.MESH
NT = (((1,), (1,)), ((), ()))


def mod(value, n):
    return lax.rem(value, n)


def device(x, y, z, core):
    return {"occ": 2 * x + lax.div(z, 4), "vir": 2 * mod(z, 4) + core, "aux": y}


def kernel(
    amp, pmask_h, left_h, lmask_h, right_h, rmask_h, out_ref,
    left, raw, rows, rside, tau0, tau1, tau2, tau3, pmask_v, lmask_v, rmask_v, qm, pmx, pm, tw, parts,
    grid_acc, part, got_xy, got_z, mine_z,
    local_sem, ring_send, ring_recv, pair_send, pair_recv,
    tx_send, tx_recv, ty_send, ty_recv, pm_send, pm_recv,
    xy_send, xy_recv, z_send, z_recv,
):
    occ, vir, y = lax.axis_index("occ"), lax.axis_index("vir"), lax.axis_index("aux")
    x, z, core = lax.div(occ, 2), mod(occ, 2) * 4 + lax.div(vir, 2), mod(vir, 2)
    here = pl.multiple_of(core * 16, 16)
    mine = pl.ds(pl.multiple_of(x * 256, 256), 256)

    tau = (tau0, tau1, tau2, tau3)

    own_right = pltpu.make_async_copy(right_h, raw, local_sem.at[4])
    own_tau = pltpu.make_async_copy(amp.at[:, :, mine], tau0, local_sem.at[5])
    small = [
        pltpu.make_async_copy(pmask_h, pmask_v, local_sem.at[6]),
        pltpu.make_async_copy(lmask_h, lmask_v, local_sem.at[7]),
        pltpu.make_async_copy(rmask_h, rmask_v, local_sem.at[8]),
    ]
    loads = [
        pltpu.make_async_copy(
            left_h.at[pl.ds(k * 8, 8)], left.at[pl.ds(k * 8, 8), :, pl.ds(0, 1024)],
            local_sem.at[k])
        for k in range(4)
    ]
    own_right.start()
    for copy in small:
        copy.start()
    for copy in loads:
        copy.start()
    own_tau.start()

    barrier = pltpu.get_barrier_semaphore()
    others = [device(mod(x + dx, NX), mod(y + dy, NY), z, core)
              for dx in range(NX) for dy in range(NY) if dx or dy]
    others += [device(x, y, mod(z + dz, NZ), core) for dz in (1, NZ - 1)]
    others += [{"occ": occ, "vir": mod(vir + dv, 8), "aux": y} for dv in range(1, 8)]
    for other in others:
        pl.semaphore_signal(barrier, inc=1, device_id=other, device_id_type=MESH)

    own_right.wait()
    wide = raw[...].astype(F32)
    for b in range(4):
        rows[b, pl.ds(32 + here, 16), :] = wide[:, b, :].astype(BF)
    for copy in small:
        copy.wait()
    tiles = (rmask_v[...] * lmask_v[...]).astype(F32)
    for q in range(8):
        qm[:, q * 128: q * 128 + 128] = jnp.broadcast_to(tiles[:, q: q + 1], (8, 128))
    ptile = pmask_v[...].reshape(8, 8).astype(F32)
    for t in range(8):
        pmx[t // 2, :, (t % 2) * 128: (t % 2) * 128 + 128] = jnp.broadcast_to(
            ptile[:, t: t + 1], (8, 128))
    pl.semaphore_wait(barrier, len(others))

    sent = []

    def go(make, *args):
        make(*args).start()
        sent.append((make, args))

    def ring(way, step, b):
        src_i, dst_i = ((1 - step) % 8, (-step) % 8) if way == 0 else (1 + step, step + 2)
        to = mod(z + 1, NZ) if way == 0 else mod(z + NZ - 1, NZ)
        return pltpu.make_async_remote_copy(
            src_ref=rows.at[b, pl.ds(src_i * 32 + here, 16), :],
            dst_ref=rows.at[b, pl.ds(dst_i * 32 + here, 16), :],
            send_sem=ring_send.at[way, step, b], recv_sem=ring_recv.at[way, step, b],
            device_id=device(x, y, to, core), device_id_type=MESH)

    def pair(i):
        return pltpu.make_async_remote_copy(
            src_ref=rows.at[:, pl.ds(i * 32 + here, 16), :],
            dst_ref=rows.at[:, pl.ds(i * 32 + here, 16), :],
            send_sem=pair_send.at[i], recv_sem=pair_recv.at[i],
            device_id=device(x, y, z, 1 - core), device_id_type=MESH)

    def tau_x(dx, first, size):
        to = mod(x + dx, NX)
        return pltpu.make_async_remote_copy(
            src_ref=amp.at[pl.ds(first, size), :, pl.ds(pl.multiple_of(to * 256, 256), 256)],
            dst_ref=tau[(-dx) % 4].at[pl.ds(first, size)],
            send_sem=tx_send.at[dx], recv_sem=tx_recv.at[dx],
            device_id=device(to, y, z, core), device_id_type=MESH)

    def tau_y(dy):
        return pltpu.make_async_remote_copy(
            src_ref=tau2.at[pl.ds(2 * y, 2)], dst_ref=tau2.at[pl.ds(2 * y, 2)],
            send_sem=ty_send.at[dy], recv_sem=ty_recv.at[dy],
            device_id=device(x, mod(y + dy, NY), z, core), device_id_type=MESH)

    def mask_x(dx):
        to = mod(x + dx, NX)
        return pltpu.make_async_remote_copy(
            src_ref=pmx.at[to], dst_ref=pm.at[(-dx) % 4],
            send_sem=pm_send.at[dx], recv_sem=pm_recv.at[dx],
            device_id=device(to, y, z, core), device_id_type=MESH)

    SPAN = {1: (0, 8), 2: (2 * y, 2), 3: (0, 8)}
    for b in range(4):
        for way in (0, 1):
            go(ring, way, 0, b)
        if b == 0:
            go(pair, 1)
    for dx in (1, 2, 3):
        go(mask_x, dx)
    go(tau_x, 2, *SPAN[2])

    def arrived(way, step, b):
        ring(way, step, b).wait_recv()
        if step < 2 or (step == 2 and (b < 2) == (way == 0)):
            go(ring, way, step + 1, b)

    def passed(step):
        for b in range(4):
            for way in (0, 1):
                if step < 3 or (b < 2) == (way == 0):
                    arrived(way, step, b)

    def across(*chips):
        for i in chips:
            go(pair, i)

    def turn(slot):
        shift = mod(9 - z, 8) * 32

        def two(step, _):
            parts = []
            for k in range(2):
                p = step * 2 + k
                mask = (pmx[x, pl.ds(p, 1), :] if slot == 0 else pm[slot, pl.ds(p, 1), :])
                parts.append(pltpu.roll(tau[slot][p].astype(F32) * mask, shift, 1))
            first = pl.multiple_of(slot * 64 + step * 16, 16)
            for odd in range(2):
                if odd:
                    parts = [jnp.concatenate(
                        [pltpu.roll(v[:, h * 128: h * 128 + 128], 64, 1) for h in range(2)],
                        axis=1) for v in parts]
                for g in range(16):
                    both = jnp.concatenate([v[g * 8: g * 8 + 8, :] for v in parts], axis=0)
                    tw[odd, g, pl.ds(first, 16), :] = both.astype(BF)
            return 0

        lax.fori_loop(0, 4, two, 0)

    def gather(m, first, place):
        for k in range(2):
            pair(first + k).wait_recv()
        for k in range(2):
            i = first + k
            row = qm[pl.ds(2 * x + lax.div(mod(z + i + 7, NZ), 4), 1), :].astype(BF)
            from_row = pl.multiple_of(i * 32, 32)
            for at in range(4):
                b = (at // 2) * 2 + mod(at + place, 2)
                rside[at * 64 + k * 32: at * 64 + k * 32 + 32, :] = (
                    rows[b, pl.ds(from_row, 32), :] * row)

    def couple(h, place, block):
        lhs = left[pl.ds(block * 8, 8), :, 0:1024].reshape(8 * 128, 1024)
        prod = lax.dot_general(lhs, rside[...], NT, preferred_element_type=F32)
        for pair_a in range(4):
            for g in range(16):
                at_a = pair_a * 256 + g * 8
                blk = jnp.concatenate(
                    [prod[at_a: at_a + 8, :], prod[at_a + 128: at_a + 136, :]], axis=0)
                hi = blk.astype(BF)
                lo = (blk - hi.astype(F32)).astype(BF)
                for at in range(4):
                    lane = (at % 2) * 64
                    for low, value in ((0, hi), (512, lo)):
                        top = pl.multiple_of(
                            low + (at // 2) * 256 + block * 64 + pair_a * 16, 16)
                        parts[h, g, mod(at + place, 2), pl.ds(top, 16), lane: lane + 64] = (
                            value[:, at * 64: at * 64 + 64])

    own_tau.wait()
    turn(0)
    for copy in loads:
        copy.wait()
    passed(0)
    across(0, 2)
    go(tau_x, 1, *SPAN[1])
    go(tau_x, 3, *SPAN[3])
    tau_x(2, *SPAN[2]).wait_recv()
    for dy in (2, 1, 3):
        go(tau_y, dy)

    def chunk(m, _):
        h = lax.div(m, 2)
        place = mod(h + m, 2)
        gather(m, 2 * m + h * (10 - 4 * m), place)

        def two(k, _):
            couple(h, place, 2 * k)
            couple(h, place, 2 * k + 1)
            return 0

        lax.fori_loop(0, 2, two, 0)

        @pl.when(m == 0)
        def _():
            passed(1)
            across(3, 7)

        @pl.when(m == 1)
        def _():
            passed(2)
            across(4, 6)
            for dx in (1, 2, 3):
                mask_x(dx).wait_recv()
            for dy in (1, 2, 3):
                tau_y(dy).wait_recv()
            turn(2)

        @pl.when(m == 2)
        def _():
            passed(3)
            across(5)
            tau_x(3, *SPAN[3]).wait_recv()
            turn(1)
            tau_x(1, *SPAN[1]).wait_recv()
            turn(3)

        return 0

    lax.fori_loop(0, 4, chunk, 0)

    grid_acc[...] = jnp.zeros_like(grid_acc)

    def contract(step, _):
        for odd in range(2):
            total = jnp.zeros((1024, 256), F32)
            for k in range(4):
                g = step * 4 + k
                both = jnp.concatenate([parts[0, g, odd], parts[1, g, odd]], axis=1)
                total = total + lax.dot_general(
                    both, tw[odd, g], NT, preferred_element_type=F32)
            grid_acc[odd * 512: odd * 512 + 512, :] += total[:512] + total[512:]
        return 0

    lax.fori_loop(0, 4, contract, 0)

    acc = grid_acc[...].reshape(128, 8, 256)
    same = (lax.broadcasted_iota(jnp.int32, (128, 8, 256), 2) % 8
            == lax.broadcasted_iota(jnp.int32, (128, 8, 256), 1))
    diag = jnp.where(same, acc, 0.0).sum(axis=1)
    pick = (lax.broadcasted_iota(jnp.int32, (32, 256), 1) // 8
            == lax.broadcasted_iota(jnp.int32, (32, 256), 0)).astype(F32).astype(BF)
    ladder = jnp.zeros((32, 128), F32)
    rest = diag
    for _ in range(3):
        top = rest.astype(BF)
        rest = rest - top.astype(F32)
        ladder = ladder + lax.dot_general(pick, top, NT, preferred_element_type=F32)
    part[...] = ladder.reshape(4, 8, 128)

    index = x * 4 + y
    got_xy[index] = part[0]

    def to_xy(dx, dy):
        return pltpu.make_async_remote_copy(
            src_ref=part.at[dx], dst_ref=got_xy.at[index],
            send_sem=xy_send.at[dx * 4 + dy], recv_sem=xy_recv.at[dx * 4 + dy],
            device_id=device(mod(x + dx, NX), mod(y + dy, NY), z, core), device_id_type=MESH)

    total = part[0]
    pairs = [(dx, dy) for dx in range(4) for dy in range(4) if dx or dy]
    pairs.sort(key=lambda d: -(d[0] == 2) - (d[1] == 2))
    for dx, dy in pairs:
        go(to_xy, dx, dy)
    for dx, dy in pairs:
        to_xy(dx, dy).wait_recv()
    total = got_xy[0]
    for k in range(1, 16):
        total = total + got_xy[k]
    mine_z[...] = total
    got_z[vir] = total

    def to_z(dv):
        return pltpu.make_async_remote_copy(
            src_ref=mine_z, dst_ref=got_z.at[vir],
            send_sem=z_send.at[dv], recv_sem=z_recv.at[dv],
            device_id={"occ": occ, "vir": mod(vir + dv, 8), "aux": y}, device_id_type=MESH)

    for dv in range(1, 8):
        go(to_z, dv)
    for dv in range(1, 8):
        to_z(dv).wait_recv()
    total = got_z[0]
    for k in range(1, 8):
        total = total + got_z[k]
    for at, b in enumerate((0, 2, 1, 3)):
        out_ref[pl.ds(b, 8, stride=4), :] = total[:, at * 32: at * 32 + 32]
    for make, args in sent:
        make(*args).wait_send()


def local(amplitudes, pair_mask, left_factor, left_mask, right_factor, right_mask, residual_in):
    dma = pltpu.SemaphoreType.DMA
    vmem = pltpu.VMEM
    ladder = pl.pallas_call(
        kernel,
        out_shape=jax.ShapeDtypeStruct((32, 32), F32),
        in_specs=[pl.BlockSpec(memory_space=pl.ANY)] * 6,
        out_specs=pl.BlockSpec(memory_space=pltpu.VMEM),
        scratch_shapes=[
            vmem((32, 128, 1152), BF),
            vmem((16, 4, 1024), BF),
            vmem((4, 256, 1024), BF),
            vmem((256, 1024), BF),
            vmem((8, 128, 256), BF), vmem((8, 128, 256), BF),
            vmem((8, 128, 256), BF), vmem((8, 128, 256), BF),
            vmem((8, 1, 8), jnp.int32),
            vmem((1, 8), jnp.int32),
            vmem((8, 8), jnp.int32),
            vmem((8, 1024), F32),
            vmem((4, 8, 256), F32),
            vmem((4, 8, 256), F32),
            vmem((2, 16, 256, 256), BF),
            vmem((2, 16, 2, 1024, 128), BF),
            vmem((1024, 256), F32),
            vmem((4, 8, 128), F32),
            vmem((16, 8, 128), F32),
            vmem((8, 8, 128), F32),
            vmem((8, 128), F32),
            dma((9,)),
            dma((2, 4, 4)), dma((2, 4, 4)),
            dma((8,)), dma((8,)),
            dma((4,)), dma((4,)),
            dma((4,)), dma((4,)),
            dma((4,)), dma((4,)),
            dma((16,)), dma((16,)),
            dma((8,)), dma((8,)),
        ],
        compiler_params=pltpu.CompilerParams(
            collective_id=0, has_side_effects=True, vmem_limit_bytes=62 * 1024 * 1024),
        name="ladder",
    )(amplitudes, pair_mask, left_factor, left_mask, right_factor, right_mask)
    return residual_in + ladder.reshape(residual_in.shape)


def solution(mesh):
    return jax.shard_map(
        local,
        mesh=mesh,
        in_specs=(
            P("occ", "vir", None),
            P("occ", "vir", None),
            P(None, "vir", "aux"),
            P("vir", "aux"),
            P(("occ", "vir"), None, "aux"),
            P(None, "aux"),
            P("occ", None, None),
        ),
        out_specs=P("occ", None, None),
        check_vma=False,
    )
```

```python
import jax
import jax.numpy as jnp
from jax import lax
from jax.experimental import pallas as pl
from jax.experimental.pallas import tpu as pltpu
from jax.sharding import PartitionSpec as P

NX, NY, NZ = 4, 4, 8
BF, F32 = jnp.bfloat16, jnp.float32
MESH = pl.DeviceIdType.MESH
NT = (((1,), (1,)), ((), ()))


def mod(value, n):
    return lax.rem(value, n)


def device(x, y, z, core):
    return {"occ": 2 * x + lax.div(z, 4), "vir": 2 * mod(z, 4) + core, "aux": y}


def kernel(
    amp, pmask_h, left_h, lmask_h, right_h, rmask_h, out_ref,
    left, raw, rows, rside, tau0, tau1, tau2, tau3, pmask_v, lmask_v, rmask_v, qm, pmx, pm, tw, parts,
    grid_acc, part, got_xy, got_z, mine_z,
    local_sem, ring_send, ring_recv, pair_send, pair_recv,
    tx_send, tx_recv, ty_send, ty_recv, pm_send, pm_recv,
    xy_send, xy_recv, z_send, z_recv,
):
    occ, vir, y = lax.axis_index("occ"), lax.axis_index("vir"), lax.axis_index("aux")
    x, z, core = lax.div(occ, 2), mod(occ, 2) * 4 + lax.div(vir, 2), mod(vir, 2)
    here = pl.multiple_of(core * 16, 16)
    mine = pl.ds(pl.multiple_of(x * 256, 256), 256)

    tau = (tau0, tau1, tau2, tau3)

    own_right = pltpu.make_async_copy(right_h, raw, local_sem.at[4])
    own_tau = pltpu.make_async_copy(amp.at[:, :, mine], tau0, local_sem.at[5])
    small = [
        pltpu.make_async_copy(pmask_h, pmask_v, local_sem.at[6]),
        pltpu.make_async_copy(lmask_h, lmask_v, local_sem.at[7]),
        pltpu.make_async_copy(rmask_h, rmask_v, local_sem.at[8]),
    ]
    loads = [
        pltpu.make_async_copy(
            left_h.at[pl.ds(k * 8, 8)], left.at[pl.ds(k * 8, 8), :, pl.ds(0, 1024)],
            local_sem.at[k])
        for k in range(4)
    ]
    own_right.start()
    for copy in small:
        copy.start()
    for copy in loads:
        copy.start()
    own_tau.start()

    barrier = pltpu.get_barrier_semaphore()
    others = [device(mod(x + dx, NX), mod(y + dy, NY), z, core)
              for dx in range(NX) for dy in range(NY) if dx or dy]
    others += [device(x, y, mod(z + dz, NZ), core) for dz in (1, NZ - 1)]
    others += [{"occ": occ, "vir": mod(vir + dv, 8), "aux": y} for dv in range(1, 8)]
    for other in others:
        pl.semaphore_signal(barrier, inc=1, device_id=other, device_id_type=MESH)

    own_right.wait()
    wide = raw[...].astype(F32)
    for b in range(4):
        rows[b, pl.ds(32 + here, 16), :] = wide[:, b, :].astype(BF)
    for copy in small:
        copy.wait()
    tiles = (rmask_v[...] * lmask_v[...]).astype(F32)
    for q in range(8):
        qm[:, q * 128: q * 128 + 128] = jnp.broadcast_to(tiles[:, q: q + 1], (8, 128))
    ptile = pmask_v[...].reshape(8, 8).astype(F32)
    for t in range(8):
        pmx[t // 2, :, (t % 2) * 128: (t % 2) * 128 + 128] = jnp.broadcast_to(
            ptile[:, t: t + 1], (8, 128))
    pl.semaphore_wait(barrier, len(others))

    sent = []

    def go(make, *args):
        make(*args).start()
        sent.append((make, args))

    def ring(way, step, b):
        src_i, dst_i = ((1 - step) % 8, (-step) % 8) if way == 0 else (1 + step, step + 2)
        to = mod(z + 1, NZ) if way == 0 else mod(z + NZ - 1, NZ)
        return pltpu.make_async_remote_copy(
            src_ref=rows.at[b, pl.ds(src_i * 32 + here, 16), :],
            dst_ref=rows.at[b, pl.ds(dst_i * 32 + here, 16), :],
            send_sem=ring_send.at[way, step, b], recv_sem=ring_recv.at[way, step, b],
            device_id=device(x, y, to, core), device_id_type=MESH)

    def pair(i):
        return pltpu.make_async_remote_copy(
            src_ref=rows.at[:, pl.ds(i * 32 + here, 16), :],
            dst_ref=rows.at[:, pl.ds(i * 32 + here, 16), :],
            send_sem=pair_send.at[i], recv_sem=pair_recv.at[i],
            device_id=device(x, y, z, 1 - core), device_id_type=MESH)

    def tau_x(dx, first, size):
        to = mod(x + dx, NX)
        return pltpu.make_async_remote_copy(
            src_ref=amp.at[pl.ds(first, size), :, pl.ds(pl.multiple_of(to * 256, 256), 256)],
            dst_ref=tau[(-dx) % 4].at[pl.ds(first, size)],
            send_sem=tx_send.at[dx], recv_sem=tx_recv.at[dx],
            device_id=device(to, y, z, core), device_id_type=MESH)

    def tau_y(dy):
        return pltpu.make_async_remote_copy(
            src_ref=tau2.at[pl.ds(2 * y, 2)], dst_ref=tau2.at[pl.ds(2 * y, 2)],
            send_sem=ty_send.at[dy], recv_sem=ty_recv.at[dy],
            device_id=device(x, mod(y + dy, NY), z, core), device_id_type=MESH)

    def mask_x(dx):
        to = mod(x + dx, NX)
        return pltpu.make_async_remote_copy(
            src_ref=pmx.at[to], dst_ref=pm.at[(-dx) % 4],
            send_sem=pm_send.at[dx], recv_sem=pm_recv.at[dx],
            device_id=device(to, y, z, core), device_id_type=MESH)

    SPAN = {1: (0, 8), 2: (2 * y, 2), 3: (0, 8)}
    for b in range(4):
        for way in (0, 1):
            go(ring, way, 0, b)
        if b == 0:
            go(pair, 1)
    for dx in (1, 2, 3):
        go(mask_x, dx)
    go(tau_x, 2, *SPAN[2])

    def arrived(way, step, b):
        ring(way, step, b).wait_recv()
        if step < 2 or (step == 2 and (b < 2) == (way == 0)):
            go(ring, way, step + 1, b)

    def passed(step):
        for b in range(4):
            for way in (0, 1):
                if step < 3 or (b < 2) == (way == 0):
                    arrived(way, step, b)

    def across(*chips):
        for i in chips:
            go(pair, i)

    def turn(slot):
        shift = mod(9 - z, 8) * 32

        def two(step, _):
            parts = []
            for k in range(2):
                p = step * 2 + k
                mask = (pmx[x, pl.ds(p, 1), :] if slot == 0 else pm[slot, pl.ds(p, 1), :])
                parts.append(pltpu.roll(tau[slot][p].astype(F32) * mask, shift, 1))
            first = pl.multiple_of(slot * 64 + step * 16, 16)
            for odd in range(2):
                if odd:
                    parts = [jnp.concatenate(
                        [pltpu.roll(v[:, h * 128: h * 128 + 128], 64, 1) for h in range(2)],
                        axis=1) for v in parts]
                for g in range(16):
                    both = jnp.concatenate([v[g * 8: g * 8 + 8, :] for v in parts], axis=0)
                    tw[odd, g, pl.ds(first, 16), :] = both.astype(BF)
            return 0

        lax.fori_loop(0, 4, two, 0)

    def gather(m, first, place):
        for k in range(2):
            pair(first + k).wait_recv()
        for k in range(2):
            i = first + k
            row = qm[pl.ds(2 * x + lax.div(mod(z + i + 7, NZ), 4), 1), :].astype(BF)
            from_row = pl.multiple_of(i * 32, 32)
            for at in range(4):
                b = (at // 2) * 2 + mod(at + place, 2)
                rside[at * 64 + k * 32: at * 64 + k * 32 + 32, :] = (
                    rows[b, pl.ds(from_row, 32), :] * row)

    def couple(h, place, block):
        lhs = left[pl.ds(block * 8, 8), :, 0:1024].reshape(8 * 128, 1024)
        prod = lax.dot_general(lhs, rside[...], NT, preferred_element_type=F32)
        for pair_a in range(4):
            for g in range(16):
                at_a = pair_a * 256 + g * 8
                blk = jnp.concatenate(
                    [prod[at_a: at_a + 8, :], prod[at_a + 128: at_a + 136, :]], axis=0)
                hi = blk.astype(BF)
                lo = (blk - hi.astype(F32)).astype(BF)
                for at in range(4):
                    lane = (at % 2) * 64
                    for low, value in ((0, hi), (512, lo)):
                        top = pl.multiple_of(
                            low + (at // 2) * 256 + block * 64 + pair_a * 16, 16)
                        parts[h, g, mod(at + place, 2), pl.ds(top, 16), lane: lane + 64] = (
                            value[:, at * 64: at * 64 + 64])

    own_tau.wait()
    turn(0)
    for copy in loads:
        copy.wait()
    passed(0)
    across(0, 2)
    go(tau_x, 1, *SPAN[1])
    go(tau_x, 3, *SPAN[3])
    tau_x(2, *SPAN[2]).wait_recv()
    for dy in (2, 1, 3):
        go(tau_y, dy)

    def chunk(m, _):
        h = lax.div(m, 2)
        place = mod(h + m, 2)
        gather(m, 2 * m + h * (10 - 4 * m), place)

        def two(k, _):
            couple(h, place, 2 * k)
            couple(h, place, 2 * k + 1)
            for step, chips in ((1, (3, 7)), (2, (4, 6)), (3, (5,))):
                @pl.when(2 * m + k == 2 * step - 2)
                def _():
                    passed(step)
                    across(*chips)

            return 0

        lax.fori_loop(0, 2, two, 0)

        @pl.when(m == 1)
        def _():
            for dx in (1, 2, 3):
                mask_x(dx).wait_recv()
            for dy in (1, 2, 3):
                tau_y(dy).wait_recv()
            turn(2)

        @pl.when(m == 2)
        def _():
            tau_x(3, *SPAN[3]).wait_recv()
            turn(1)
            tau_x(1, *SPAN[1]).wait_recv()
            turn(3)

        return 0

    lax.fori_loop(0, 4, chunk, 0)

    grid_acc[...] = jnp.zeros_like(grid_acc)

    def contract(step, _):
        for odd in range(2):
            total = jnp.zeros((1024, 256), F32)
            for k in range(4):
                g = step * 4 + k
                both = jnp.concatenate([parts[0, g, odd], parts[1, g, odd]], axis=1)
                total = total + lax.dot_general(
                    both, tw[odd, g], NT, preferred_element_type=F32)
            grid_acc[odd * 512: odd * 512 + 512, :] += total[:512] + total[512:]
        return 0

    lax.fori_loop(0, 4, contract, 0)

    acc = grid_acc[...].reshape(128, 8, 256)
    same = (lax.broadcasted_iota(jnp.int32, (128, 8, 256), 2) % 8
            == lax.broadcasted_iota(jnp.int32, (128, 8, 256), 1))
    diag = jnp.where(same, acc, 0.0).sum(axis=1)
    pick = (lax.broadcasted_iota(jnp.int32, (32, 256), 1) // 8
            == lax.broadcasted_iota(jnp.int32, (32, 256), 0)).astype(F32).astype(BF)
    ladder = jnp.zeros((32, 128), F32)
    rest = diag
    for _ in range(3):
        top = rest.astype(BF)
        rest = rest - top.astype(F32)
        ladder = ladder + lax.dot_general(pick, top, NT, preferred_element_type=F32)
    part[...] = ladder.reshape(4, 8, 128)

    index = x * 4 + y
    got_xy[index] = part[0]

    def to_xy(dx, dy):
        return pltpu.make_async_remote_copy(
            src_ref=part.at[dx], dst_ref=got_xy.at[index],
            send_sem=xy_send.at[dx * 4 + dy], recv_sem=xy_recv.at[dx * 4 + dy],
            device_id=device(mod(x + dx, NX), mod(y + dy, NY), z, core), device_id_type=MESH)

    total = part[0]
    pairs = [(dx, dy) for dx in range(4) for dy in range(4) if dx or dy]
    pairs.sort(key=lambda d: -(d[0] == 2) - (d[1] == 2))
    for dx, dy in pairs:
        go(to_xy, dx, dy)
    for dx, dy in pairs:
        to_xy(dx, dy).wait_recv()
    total = got_xy[0]
    for k in range(1, 16):
        total = total + got_xy[k]
    mine_z[...] = total
    got_z[vir] = total

    def to_z(dv):
        return pltpu.make_async_remote_copy(
            src_ref=mine_z, dst_ref=got_z.at[vir],
            send_sem=z_send.at[dv], recv_sem=z_recv.at[dv],
            device_id={"occ": occ, "vir": mod(vir + dv, 8), "aux": y}, device_id_type=MESH)

    for dv in range(1, 8):
        go(to_z, dv)
    for dv in range(1, 8):
        to_z(dv).wait_recv()
    total = got_z[0]
    for k in range(1, 8):
        total = total + got_z[k]
    for at, b in enumerate((0, 2, 1, 3)):
        out_ref[pl.ds(b, 8, stride=4), :] = total[:, at * 32: at * 32 + 32]
    for make, args in sent:
        make(*args).wait_send()


def local(amplitudes, pair_mask, left_factor, left_mask, right_factor, right_mask, residual_in):
    dma = pltpu.SemaphoreType.DMA
    vmem = pltpu.VMEM
    ladder = pl.pallas_call(
        kernel,
        out_shape=jax.ShapeDtypeStruct((32, 32), F32),
        in_specs=[pl.BlockSpec(memory_space=pl.ANY)] * 6,
        out_specs=pl.BlockSpec(memory_space=pltpu.VMEM),
        scratch_shapes=[
            vmem((32, 128, 1152), BF),
            vmem((16, 4, 1024), BF),
            vmem((4, 256, 1024), BF),
            vmem((256, 1024), BF),
            vmem((8, 128, 256), BF), vmem((8, 128, 256), BF),
            vmem((8, 128, 256), BF), vmem((8, 128, 256), BF),
            vmem((8, 1, 8), jnp.int32),
            vmem((1, 8), jnp.int32),
            vmem((8, 8), jnp.int32),
            vmem((8, 1024), F32),
            vmem((4, 8, 256), F32),
            vmem((4, 8, 256), F32),
            vmem((2, 16, 256, 256), BF),
            vmem((2, 16, 2, 1024, 128), BF),
            vmem((1024, 256), F32),
            vmem((4, 8, 128), F32),
            vmem((16, 8, 128), F32),
            vmem((8, 8, 128), F32),
            vmem((8, 128), F32),
            dma((9,)),
            dma((2, 4, 4)), dma((2, 4, 4)),
            dma((8,)), dma((8,)),
            dma((4,)), dma((4,)),
            dma((4,)), dma((4,)),
            dma((4,)), dma((4,)),
            dma((16,)), dma((16,)),
            dma((8,)), dma((8,)),
        ],
        compiler_params=pltpu.CompilerParams(
            collective_id=0, has_side_effects=True, vmem_limit_bytes=62 * 1024 * 1024),
        name="ladder",
    )(amplitudes, pair_mask, left_factor, left_mask, right_factor, right_mask)
    return residual_in + ladder.reshape(residual_in.shape)


def solution(mesh):
    return jax.shard_map(
        local,
        mesh=mesh,
        in_specs=(
            P("occ", "vir", None),
            P("occ", "vir", None),
            P(None, "vir", "aux"),
            P("vir", "aux"),
            P(("occ", "vir"), None, "aux"),
            P(None, "aux"),
            P("occ", None, None),
        ),
        out_specs=P("occ", None, None),
        check_vma=False,
    )
```

```python
import jax
import jax.numpy as jnp
from jax import lax
from jax.experimental import pallas as pl
from jax.experimental.pallas import tpu as pltpu
from jax.sharding import PartitionSpec as P

NX, NY, NZ = 4, 4, 8
BF, F32 = jnp.bfloat16, jnp.float32
MESH = pl.DeviceIdType.MESH
NT = (((1,), (1,)), ((), ()))


def mod(value, n):
    return lax.rem(value, n)


def device(x, y, z, core):
    return {"occ": 2 * x + lax.div(z, 4), "vir": 2 * mod(z, 4) + core, "aux": y}


def kernel(
    amp, pmask_h, left_h, lmask_h, right_h, rmask_h, out_ref,
    left, raw, rows, rside, tau0, tau1, tau2, tau3, pmask_v, lmask_v, rmask_v, qm, pmx, pm, tw, parts,
    grid_acc, part, got_xy, got_z, mine_z,
    local_sem, ring_send, ring_recv, pair_send, pair_recv,
    tx_send, tx_recv, ty_send, ty_recv, pm_send, pm_recv,
    xy_send, xy_recv, z_send, z_recv,
):
    occ, vir, y = lax.axis_index("occ"), lax.axis_index("vir"), lax.axis_index("aux")
    x, z, core = lax.div(occ, 2), mod(occ, 2) * 4 + lax.div(vir, 2), mod(vir, 2)
    here = pl.multiple_of(core * 16, 16)
    mine = pl.ds(pl.multiple_of(x * 256, 256), 256)

    tau = (tau0, tau1, tau2, tau3)

    own_right = pltpu.make_async_copy(right_h, raw, local_sem.at[4])
    own_tau = pltpu.make_async_copy(amp.at[:, :, mine], tau0, local_sem.at[5])
    small = [
        pltpu.make_async_copy(pmask_h, pmask_v, local_sem.at[6]),
        pltpu.make_async_copy(lmask_h, lmask_v, local_sem.at[7]),
        pltpu.make_async_copy(rmask_h, rmask_v, local_sem.at[8]),
    ]
    loads = [
        pltpu.make_async_copy(
            left_h.at[pl.ds(k * 8, 8)], left.at[pl.ds(k * 8, 8), :, pl.ds(0, 1024)],
            local_sem.at[k])
        for k in range(4)
    ]
    own_right.start()
    for copy in small:
        copy.start()
    for copy in loads:
        copy.start()
    own_tau.start()

    barrier = pltpu.get_barrier_semaphore()
    others = [device(mod(x + dx, NX), mod(y + dy, NY), z, core)
              for dx in range(NX) for dy in range(NY) if (dx == 0) != (dy == 0)]
    others += [device(x, y, mod(z + dz, NZ), core) for dz in (1, NZ - 1)]
    others += [device(x, y, z, 1 - core)]
    for other in others:
        pl.semaphore_signal(barrier, inc=1, device_id=other, device_id_type=MESH)

    own_right.wait()
    wide = raw[...].astype(F32)
    for b in range(4):
        rows[b, pl.ds(32 + here, 16), :] = wide[:, b, :].astype(BF)
    for copy in small:
        copy.wait()
    tiles = (rmask_v[...] * lmask_v[...]).astype(F32)
    for q in range(8):
        qm[:, q * 128: q * 128 + 128] = jnp.broadcast_to(tiles[:, q: q + 1], (8, 128))
    ptile = pmask_v[...].reshape(8, 8).astype(F32)
    for t in range(8):
        pmx[t // 2, :, (t % 2) * 128: (t % 2) * 128 + 128] = jnp.broadcast_to(
            ptile[:, t: t + 1], (8, 128))
    pl.semaphore_wait(barrier, len(others))

    sent = []

    def go(make, *args):
        make(*args).start()
        sent.append((make, args))

    def ring(way, step, b):
        src_i, dst_i = ((1 - step) % 8, (-step) % 8) if way == 0 else (1 + step, step + 2)
        to = mod(z + 1, NZ) if way == 0 else mod(z + NZ - 1, NZ)
        return pltpu.make_async_remote_copy(
            src_ref=rows.at[b, pl.ds(src_i * 32 + here, 16), :],
            dst_ref=rows.at[b, pl.ds(dst_i * 32 + here, 16), :],
            send_sem=ring_send.at[way, step, b], recv_sem=ring_recv.at[way, step, b],
            device_id=device(x, y, to, core), device_id_type=MESH)

    def pair(i):
        return pltpu.make_async_remote_copy(
            src_ref=rows.at[:, pl.ds(i * 32 + here, 16), :],
            dst_ref=rows.at[:, pl.ds(i * 32 + here, 16), :],
            send_sem=pair_send.at[i], recv_sem=pair_recv.at[i],
            device_id=device(x, y, z, 1 - core), device_id_type=MESH)

    def tau_x(dx, first, size):
        to = mod(x + dx, NX)
        return pltpu.make_async_remote_copy(
            src_ref=amp.at[pl.ds(first, size), :, pl.ds(pl.multiple_of(to * 256, 256), 256)],
            dst_ref=tau[(-dx) % 4].at[pl.ds(first, size)],
            send_sem=tx_send.at[dx], recv_sem=tx_recv.at[dx],
            device_id=device(to, y, z, core), device_id_type=MESH)

    def tau_y(dy):
        return pltpu.make_async_remote_copy(
            src_ref=tau2.at[pl.ds(2 * y, 2)], dst_ref=tau2.at[pl.ds(2 * y, 2)],
            send_sem=ty_send.at[dy], recv_sem=ty_recv.at[dy],
            device_id=device(x, mod(y + dy, NY), z, core), device_id_type=MESH)

    def mask_x(dx):
        to = mod(x + dx, NX)
        return pltpu.make_async_remote_copy(
            src_ref=pmx.at[to], dst_ref=pm.at[(-dx) % 4],
            send_sem=pm_send.at[dx], recv_sem=pm_recv.at[dx],
            device_id=device(to, y, z, core), device_id_type=MESH)

    SPAN = {1: (0, 8), 2: (2 * y, 2), 3: (0, 8)}
    for b in range(4):
        for way in (0, 1):
            go(ring, way, 0, b)
        if b == 0:
            go(pair, 1)
    for dx in (1, 2, 3):
        go(mask_x, dx)
    go(tau_x, 2, *SPAN[2])

    def arrived(way, step, b):
        ring(way, step, b).wait_recv()
        if step < 2 or (step == 2 and (b < 2) == (way == 0)):
            go(ring, way, step + 1, b)

    def passed(step):
        for b in range(4):
            for way in (0, 1):
                if step < 3 or (b < 2) == (way == 0):
                    arrived(way, step, b)

    def across(*chips):
        for i in chips:
            go(pair, i)

    def turn(slot):
        shift = mod(9 - z, 8) * 32

        def two(step, _):
            parts = []
            for k in range(2):
                p = step * 2 + k
                mask = (pmx[x, pl.ds(p, 1), :] if slot == 0 else pm[slot, pl.ds(p, 1), :])
                parts.append(pltpu.roll(tau[slot][p].astype(F32) * mask, shift, 1))
            first = pl.multiple_of(slot * 64 + step * 16, 16)
            for odd in range(2):
                if odd:
                    parts = [jnp.concatenate(
                        [pltpu.roll(v[:, h * 128: h * 128 + 128], 64, 1) for h in range(2)],
                        axis=1) for v in parts]
                for g in range(16):
                    both = jnp.concatenate([v[g * 8: g * 8 + 8, :] for v in parts], axis=0)
                    tw[odd, g, pl.ds(first, 16), :] = both.astype(BF)
            return 0

        lax.fori_loop(0, 4, two, 0)

    def gather(m, first, place):
        for k in range(2):
            pair(first + k).wait_recv()
        for k in range(2):
            i = first + k
            row = qm[pl.ds(2 * x + lax.div(mod(z + i + 7, NZ), 4), 1), :].astype(BF)
            from_row = pl.multiple_of(i * 32, 32)
            for at in range(4):
                b = (at // 2) * 2 + mod(at + place, 2)
                rside[at * 64 + k * 32: at * 64 + k * 32 + 32, :] = (
                    rows[b, pl.ds(from_row, 32), :] * row)

    def couple(h, place, block):
        lhs = left[pl.ds(block * 8, 8), :, 0:1024].reshape(8 * 128, 1024)
        prod = lax.dot_general(lhs, rside[...], NT, preferred_element_type=F32)
        for pair_a in range(4):
            for g in range(16):
                at_a = pair_a * 256 + g * 8
                blk = jnp.concatenate(
                    [prod[at_a: at_a + 8, :], prod[at_a + 128: at_a + 136, :]], axis=0)
                hi = blk.astype(BF)
                lo = (blk - hi.astype(F32)).astype(BF)
                for at in range(4):
                    lane = (at % 2) * 64
                    for low, value in ((0, hi), (512, lo)):
                        top = pl.multiple_of(
                            low + (at // 2) * 256 + block * 64 + pair_a * 16, 16)
                        parts[h, g, mod(at + place, 2), pl.ds(top, 16), lane: lane + 64] = (
                            value[:, at * 64: at * 64 + 64])

    own_tau.wait()
    turn(0)
    for copy in loads:
        copy.wait()
    passed(0)
    across(0, 2)
    go(tau_x, 1, *SPAN[1])
    go(tau_x, 3, *SPAN[3])
    tau_x(2, *SPAN[2]).wait_recv()
    for dy in (2, 1, 3):
        go(tau_y, dy)

    def chunk(m, _):
        h = lax.div(m, 2)
        place = mod(h + m, 2)
        gather(m, 2 * m + h * (10 - 4 * m), place)

        def two(k, _):
            couple(h, place, 2 * k)
            couple(h, place, 2 * k + 1)
            for step, chips in ((1, (3, 7)), (2, (4, 6)), (3, (5,))):
                @pl.when(2 * m + k == 2 * step - 2)
                def _():
                    passed(step)
                    across(*chips)

            return 0

        lax.fori_loop(0, 2, two, 0)

        @pl.when(m == 1)
        def _():
            for dx in (1, 2, 3):
                mask_x(dx).wait_recv()
            for dy in (1, 2, 3):
                tau_y(dy).wait_recv()
            turn(2)

        @pl.when(m == 2)
        def _():
            tau_x(3, *SPAN[3]).wait_recv()
            turn(1)
            tau_x(1, *SPAN[1]).wait_recv()
            turn(3)

        return 0

    lax.fori_loop(0, 4, chunk, 0)

    grid_acc[...] = jnp.zeros_like(grid_acc)

    def contract(step, _):
        for odd in range(2):
            total = jnp.zeros((1024, 256), F32)
            for k in range(4):
                g = step * 4 + k
                both = jnp.concatenate([parts[0, g, odd], parts[1, g, odd]], axis=1)
                total = total + lax.dot_general(
                    both, tw[odd, g], NT, preferred_element_type=F32)
            grid_acc[odd * 512: odd * 512 + 512, :] += total[:512] + total[512:]
        return 0

    lax.fori_loop(0, 4, contract, 0)

    acc = grid_acc[...].reshape(128, 8, 256)
    same = (lax.broadcasted_iota(jnp.int32, (128, 8, 256), 2) % 8
            == lax.broadcasted_iota(jnp.int32, (128, 8, 256), 1))
    diag = jnp.where(same, acc, 0.0).sum(axis=1)
    pick = (lax.broadcasted_iota(jnp.int32, (32, 256), 1) // 8
            == lax.broadcasted_iota(jnp.int32, (32, 256), 0)).astype(F32).astype(BF)
    ladder = jnp.zeros((32, 128), F32)
    rest = diag
    for _ in range(3):
        top = rest.astype(BF)
        rest = rest - top.astype(F32)
        ladder = ladder + lax.dot_general(pick, top, NT, preferred_element_type=F32)
    part[...] = ladder.reshape(4, 8, 128)

    index = x * 4 + y
    got_xy[index] = part[0]

    def to_xy(dx, dy):
        return pltpu.make_async_remote_copy(
            src_ref=part.at[dx], dst_ref=got_xy.at[index],
            send_sem=xy_send.at[dx * 4 + dy], recv_sem=xy_recv.at[dx * 4 + dy],
            device_id=device(mod(x + dx, NX), mod(y + dy, NY), z, core), device_id_type=MESH)

    total = part[0]
    pairs = [(dx, dy) for dx in range(4) for dy in range(4) if dx or dy]
    pairs.sort(key=lambda d: -(d[0] == 2) - (d[1] == 2))
    for dx, dy in pairs:
        go(to_xy, dx, dy)
    for dx, dy in pairs:
        to_xy(dx, dy).wait_recv()
    total = got_xy[0]
    for k in range(1, 16):
        total = total + got_xy[k]
    mine_z[...] = total
    got_z[vir] = total

    def to_z(dv):
        return pltpu.make_async_remote_copy(
            src_ref=mine_z, dst_ref=got_z.at[vir],
            send_sem=z_send.at[dv], recv_sem=z_recv.at[dv],
            device_id={"occ": occ, "vir": mod(vir + dv, 8), "aux": y}, device_id_type=MESH)

    for dv in range(1, 8):
        go(to_z, dv)
    for dv in range(1, 8):
        to_z(dv).wait_recv()
    total = got_z[0]
    for k in range(1, 8):
        total = total + got_z[k]
    for at, b in enumerate((0, 2, 1, 3)):
        out_ref[pl.ds(b, 8, stride=4), :] = total[:, at * 32: at * 32 + 32]
    for make, args in sent:
        make(*args).wait_send()


def local(amplitudes, pair_mask, left_factor, left_mask, right_factor, right_mask, residual_in):
    dma = pltpu.SemaphoreType.DMA
    vmem = pltpu.VMEM
    ladder = pl.pallas_call(
        kernel,
        out_shape=jax.ShapeDtypeStruct((32, 32), F32),
        in_specs=[pl.BlockSpec(memory_space=pl.ANY)] * 6,
        out_specs=pl.BlockSpec(memory_space=pltpu.VMEM),
        scratch_shapes=[
            vmem((32, 128, 1152), BF),
            vmem((16, 4, 1024), BF),
            vmem((4, 256, 1024), BF),
            vmem((256, 1024), BF),
            vmem((8, 128, 256), BF), vmem((8, 128, 256), BF),
            vmem((8, 128, 256), BF), vmem((8, 128, 256), BF),
            vmem((8, 1, 8), jnp.int32),
            vmem((1, 8), jnp.int32),
            vmem((8, 8), jnp.int32),
            vmem((8, 1024), F32),
            vmem((4, 8, 256), F32),
            vmem((4, 8, 256), F32),
            vmem((2, 16, 256, 256), BF),
            vmem((2, 16, 2, 1024, 128), BF),
            vmem((1024, 256), F32),
            vmem((4, 8, 128), F32),
            vmem((16, 8, 128), F32),
            vmem((8, 8, 128), F32),
            vmem((8, 128), F32),
            dma((9,)),
            dma((2, 4, 4)), dma((2, 4, 4)),
            dma((8,)), dma((8,)),
            dma((4,)), dma((4,)),
            dma((4,)), dma((4,)),
            dma((4,)), dma((4,)),
            dma((16,)), dma((16,)),
            dma((8,)), dma((8,)),
        ],
        compiler_params=pltpu.CompilerParams(
            collective_id=0, has_side_effects=True, vmem_limit_bytes=62 * 1024 * 1024),
        name="ladder",
    )(amplitudes, pair_mask, left_factor, left_mask, right_factor, right_mask)
    return residual_in + ladder.reshape(residual_in.shape)


def solution(mesh):
    return jax.shard_map(
        local,
        mesh=mesh,
        in_specs=(
            P("occ", "vir", None),
            P("occ", "vir", None),
            P(None, "vir", "aux"),
            P("vir", "aux"),
            P(("occ", "vir"), None, "aux"),
            P(None, "aux"),
            P("occ", None, None),
        ),
        out_specs=P("occ", None, None),
        check_vma=False,
    )
```
